32 devices in a mesh: dp: 2 (over x), m: 4 (over z), bx: 4 (over y, core).
Axes of the slice: x: 2, y: 2, z: 4, core: 2. Of those that a mesh axis runs over, the one named last changes fastest.
Arguments:
- x_in: bfloat16 [8, 2048, 2048], P(('dp', 'bx'), None, 'm'), parts along dimension 0
- prompt_len: int32 [8], P(('dp', 'bx')), parts along dimension 0
- ln_scale: float32 [2, 2048], P(None, 'm')
- w_gate: bfloat16 [2, 2048, 16384], P(None, 'bx', 'm')
- w_up: bfloat16 [2, 2048, 16384], P(None, 'bx', 'm')
- w_q: bfloat16 [2, 2048, 8, 256], P(None, 'bx', 'm')
- w_k: bfloat16 [2, 2048, 256], P(None, 'bx')
- w_v: bfloat16 [2, 2048, 256], P(None, 'bx')
- w_down: bfloat16 [2, 16384, 2048], P(None, 'm', 'bx')
- w_o: bfloat16 [2, 8, 256, 2048], P(None, 'm', None, 'bx')
Outputs:
- output 1: bfloat16 [8, 2048, 2048], P(('dp', 'bx'), None, 'm'), parts along dimension 0
- output 2: bfloat16 [2, 8, 2048, 256], P(None, ('dp', 'bx')), parts along dimension 1
- output 3: bfloat16 [2, 8, 2048, 256], P(None, ('dp', 'bx')), parts along dimension 1
There are 2 independent parts. The reference program is written for one: setup_inputs(seed, part) draws one part's arguments, and reference() takes and returns one part's arrays. A program takes and returns all parts, laid end to end along the dimension named above; an argument that names none is the same for every part.
All inputs are finite; a program needn't handle non-finite values.
Results may differ from the reference program's by a relative error of at most 0.0138366.
Values are sent between devices in bfloat16 or wider.
A program may use at most 1 GiB of HBM per device.

```python
import jax
import jax.numpy as jnp
from jax import lax

BATCH_ROWS = 4
SEQ_LEN = 2048
EMBED_DIM = 2048
NUM_HEADS = 8
HEAD_DIM = 256
FFN_DIM = 16384
NUM_LAYERS = 2

NORM_EPS = 1e-6
ROPE_BASE = 10000.0
QUERY_BLOCK = min(SEQ_LEN, 512)
SCORE_SCALE = HEAD_DIM ** -0.5


def setup_inputs(seed: int = 0, part: int = 0) -> dict:
    base_key = jax.random.key(seed)

    def shared_normal(index, shape, fan_in):
        draw = jax.random.normal(jax.random.fold_in(base_key, index), shape, jnp.float32)
        return (draw * fan_in ** -0.5).astype(jnp.bfloat16)

    x_key = jax.random.fold_in(jax.random.fold_in(base_key, 1), part)
    x_in = jax.random.normal(x_key, (BATCH_ROWS, SEQ_LEN, EMBED_DIM), jnp.float32).astype(jnp.bfloat16)
    len_key = jax.random.fold_in(jax.random.fold_in(base_key, 2), part)
    prompt_len = jax.random.randint(len_key, (BATCH_ROWS,), SEQ_LEN // 16, SEQ_LEN + 1, dtype=jnp.int32)
    full_row = jax.random.randint(jax.random.fold_in(len_key, 1), (), 0, BATCH_ROWS)
    short_row = (full_row + jax.random.randint(jax.random.fold_in(len_key, 2), (), 1, BATCH_ROWS)) % BATCH_ROWS
    prompt_len = prompt_len.at[full_row].set(SEQ_LEN).at[short_row].set(SEQ_LEN // 16)
    ln_scale = 1.0 + 0.2 * jax.random.normal(jax.random.fold_in(base_key, 3), (NUM_LAYERS, EMBED_DIM), jnp.float32)
    return {
        'x_in': x_in,
        'prompt_len': prompt_len,
        'ln_scale': ln_scale,
        'w_gate': shared_normal(4, (NUM_LAYERS, EMBED_DIM, FFN_DIM), EMBED_DIM),
        'w_up': shared_normal(5, (NUM_LAYERS, EMBED_DIM, FFN_DIM), EMBED_DIM),
        'w_q': shared_normal(6, (NUM_LAYERS, EMBED_DIM, NUM_HEADS, HEAD_DIM), EMBED_DIM),
        'w_k': shared_normal(7, (NUM_LAYERS, EMBED_DIM, HEAD_DIM), EMBED_DIM),
        'w_v': shared_normal(8, (NUM_LAYERS, EMBED_DIM, HEAD_DIM), EMBED_DIM),
        'w_down': shared_normal(9, (NUM_LAYERS, FFN_DIM, EMBED_DIM), FFN_DIM),
        'w_o': shared_normal(10, (NUM_LAYERS, NUM_HEADS, HEAD_DIM, EMBED_DIM), NUM_HEADS * HEAD_DIM // 4),
    }


def layer_norm(x_row, scale_row):
    x_f32 = x_row.astype(jnp.float32)
    row_mean = jnp.mean(x_f32, axis=-1, keepdims=True)
    centered = x_f32 - row_mean
    row_var = jnp.mean(centered * centered, axis=-1, keepdims=True)
    return (centered * lax.rsqrt(row_var + NORM_EPS) * scale_row).astype(jnp.bfloat16)


def apply_rotary(values, cos_tab, sin_tab):
    half_dim = values.shape[-1] // 2
    first_half = values[..., :half_dim]
    second_half = values[..., half_dim:]
    return jnp.concatenate([first_half * cos_tab - second_half * sin_tab, second_half * cos_tab + first_half * sin_tab], axis=-1)


def attention_row(query_rows, key_rows, val_rows, row_len):
    block_count = SEQ_LEN // QUERY_BLOCK
    query_blocks = query_rows.reshape(block_count, QUERY_BLOCK, NUM_HEADS, HEAD_DIM)
    key_pos = jnp.arange(SEQ_LEN)
    key_f32 = key_rows.astype(jnp.float32)
    val_f32 = val_rows.astype(jnp.float32)

    def one_block(block_args):
        query_blk, block_idx = block_args
        scores = jnp.einsum('qhd,kd->hqk', query_blk.astype(jnp.float32), key_f32) * SCORE_SCALE
        query_pos = block_idx * QUERY_BLOCK + jnp.arange(QUERY_BLOCK)
        visible = (key_pos[None, :] <= query_pos[:, None]) & (key_pos[None, :] < row_len)
        scores = jnp.where(visible[None, :, :], scores, -1e30)
        attn_probs = jax.nn.softmax(scores, axis=-1).astype(jnp.bfloat16)
        block_out = jnp.einsum('hqk,kd->qhd', attn_probs.astype(jnp.float32), val_f32)
        return block_out.astype(jnp.bfloat16)

    blocks_out = lax.map(one_block, (query_blocks, jnp.arange(block_count)))
    return blocks_out.reshape(SEQ_LEN, NUM_HEADS * HEAD_DIM)


def row_forward(x_row, row_len, layer_params, cos_tab, sin_tab):
    ln_row, w_gate, w_up, w_q, w_k, w_v, w_down, w_o = layer_params
    normed = layer_norm(x_row, ln_row)
    gate_proj = jnp.dot(normed, w_gate, preferred_element_type=jnp.float32)
    up_proj = jnp.dot(normed, w_up, preferred_element_type=jnp.float32)
    act_bf = (jax.nn.silu(gate_proj) * up_proj).astype(jnp.bfloat16)
    query_lin = jnp.dot(normed, w_q.reshape(EMBED_DIM, NUM_HEADS * HEAD_DIM), preferred_element_type=jnp.float32)
    query_lin = query_lin.reshape(SEQ_LEN, NUM_HEADS, HEAD_DIM)
    query_rows = apply_rotary(query_lin, cos_tab[:, None, :], sin_tab[:, None, :]).astype(jnp.bfloat16)
    key_lin = jnp.dot(normed, w_k, preferred_element_type=jnp.float32)
    key_rows = apply_rotary(key_lin, cos_tab, sin_tab).astype(jnp.bfloat16)
    val_rows = jnp.dot(normed, w_v, preferred_element_type=jnp.float32).astype(jnp.bfloat16)
    attn_out = attention_row(query_rows, key_rows, val_rows, row_len)
    mixed_sum = jnp.dot(act_bf, w_down, preferred_element_type=jnp.float32) + jnp.dot(attn_out, w_o.reshape(NUM_HEADS * HEAD_DIM, EMBED_DIM), preferred_element_type=jnp.float32)
    y_row = (x_row.astype(jnp.float32) + mixed_sum).astype(jnp.bfloat16)
    return y_row, key_rows, val_rows


def reference(x_in, prompt_len, ln_scale, w_gate, w_up, w_q, w_k, w_v, w_down, w_o):
    half_dim = HEAD_DIM // 2
    inv_freq = ROPE_BASE ** (-jnp.arange(half_dim, dtype=jnp.float32) * (2.0 / HEAD_DIM))
    angles = jnp.arange(SEQ_LEN, dtype=jnp.float32)[:, None] * inv_freq[None, :]
    cos_tab = jnp.cos(angles)
    sin_tab = jnp.sin(angles)

    def layer_step(hidden, layer_params):
        def row_step(row_args):
            return row_forward(row_args[0], row_args[1], layer_params, cos_tab, sin_tab)
        y_rows, key_rows, val_rows = lax.map(row_step, (hidden, prompt_len))
        return y_rows, (key_rows, val_rows)

    y_out, caches = lax.scan(layer_step, x_in, (ln_scale, w_gate, w_up, w_q, w_k, w_v, w_down, w_o))
    return y_out, caches[0], caches[1]
```

```python
import functools

import jax
import jax.numpy as jnp
from jax import lax
from jax.experimental import pallas as pl
from jax.experimental.pallas import tpu as pltpu
from jax.sharding import PartitionSpec as P


NORM_EPS = 1e-6
ROPE_BASE = 10000.0
NUM_CHUNKS = 4
FFN_TILE = 512
VMEM_BYTES = 60 * 1024 * 1024


def rotary_tables(positions, head_dim):
    half_dim = head_dim // 2
    inv_freq = ROPE_BASE ** (-jnp.arange(half_dim, dtype=jnp.float32) * (2.0 / head_dim))
    angles = positions.astype(jnp.float32)[:, None] * inv_freq[None, :]
    return jnp.cos(angles), jnp.sin(angles)


def row_offsets(me, group, rows):
    half = rows // 2
    other = me ^ 1
    far = me ^ 2
    far_other = me ^ 3
    return (
        me * rows,
        other * rows,
        far * rows + group * half,
        far * rows + (1 - group) * half,
        far_other * rows + group * half,
        far_other * rows + (1 - group) * half,
    )


def piece_copies(pieces, dst, offsets, cols, sem):
    copies = []
    for piece, offset in zip(pieces, offsets):
        rows = piece.shape[0]
        copies.append(pltpu.make_async_copy(piece.at[:, cols], dst.at[pl.ds(pl.multiple_of(offset, rows), rows)], sem))
    return copies


def qkv_body(place, x_ref, ln_ref, cos_ref, sin_ref, *refs, head_dim, num_q, split):
    pieces = refs[:6]
    h_ref, q_ref, k_ref, v_ref, w_full, sem = refs[6:]
    offsets = row_offsets(place[0], place[1], pieces[0].shape[0])
    out_dim = w_full.shape[1]
    copies = piece_copies(pieces, w_full, offsets, slice(0, out_dim), sem)
    for copy in copies:
        copy.start()
    tokens, _ = h_ref.shape
    step = min(128, tokens)

    def norm_step(i, carry):
        rows = pl.ds(pl.multiple_of(i * step, step), step)
        if split:
            x = jnp.concatenate([x_ref[j, rows, :] for j in range(x_ref.shape[0])], axis=-1).astype(jnp.float32)
        else:
            x = x_ref[rows, :].astype(jnp.float32)
        mean = jnp.mean(x, axis=-1, keepdims=True)
        centered = x - mean
        var = jnp.mean(centered * centered, axis=-1, keepdims=True)
        h_ref[rows, :] = (centered * lax.rsqrt(var + NORM_EPS) * ln_ref[...]).astype(jnp.bfloat16)
        return carry

    lax.fori_loop(0, tokens // step, norm_step, 0)
    for copy in copies:
        copy.wait()
    half = head_dim // 2
    cos = cos_ref[...]
    sin = sin_ref[...]
    h = h_ref[...]
    for i in range(num_q + 2):
        lin = jnp.dot(h, w_full[:, i * head_dim:(i + 1) * head_dim], preferred_element_type=jnp.float32)
        if i == num_q + 1:
            v_ref[...] = lin.astype(jnp.bfloat16)
            continue
        u1 = lin[:, :half]
        u2 = lin[:, half:]
        lo = (u1 * cos - u2 * sin).astype(jnp.bfloat16)
        hi = (u2 * cos + u1 * sin).astype(jnp.bfloat16)
        if i < num_q:
            q_ref[:, i * head_dim:i * head_dim + half] = lo
            q_ref[:, i * head_dim + half:(i + 1) * head_dim] = hi
        else:
            k_ref[:, :half] = lo
            k_ref[:, half:] = hi


def qkv_call(place, x_chunk, ln_row, cos, sin, pieces, head_dim, num_q):
    split = x_chunk.ndim == 3
    tokens = x_chunk.shape[-2]
    embed = ln_row.shape[1]
    out_dim = (num_q + 2) * head_dim
    full = lambda shape: pl.BlockSpec(shape, lambda i, s: (0,) * len(shape))
    anyspec = pl.BlockSpec(memory_space=pl.ANY)
    bf16 = jnp.bfloat16
    return pl.pallas_call(
        functools.partial(qkv_body, head_dim=head_dim, num_q=num_q, split=split),
        grid_spec=pltpu.PrefetchScalarGridSpec(
            num_scalar_prefetch=1,
            grid=(1,),
            in_specs=[full(x_chunk.shape), full(ln_row.shape), full(cos.shape), full(sin.shape)] + [anyspec] * 6,
            out_specs=[full((tokens, embed)), full((tokens, num_q * head_dim)), full((tokens, head_dim)), full((tokens, head_dim))],
            scratch_shapes=[pltpu.VMEM((embed, out_dim), bf16), pltpu.SemaphoreType.DMA],
        ),
        out_shape=[
            jax.ShapeDtypeStruct((tokens, embed), bf16),
            jax.ShapeDtypeStruct((tokens, num_q * head_dim), bf16),
            jax.ShapeDtypeStruct((tokens, head_dim), bf16),
            jax.ShapeDtypeStruct((tokens, head_dim), bf16),
        ],
        compiler_params=pltpu.CompilerParams(vmem_limit_bytes=VMEM_BYTES),
        cost_estimate=pl.CostEstimate(flops=2 * tokens * embed * out_dim * 2, bytes_accessed=2 * (2 * tokens * embed + embed * out_dim), transcendentals=0),
        name="qkv",
    )(place, x_chunk, ln_row, cos, sin, *pieces)


def attn_body(lens, q_ref, *refs, head_dim, num_q, block):
    num_kv = (len(refs) - 1) // 2
    k_refs = refs[:num_kv]
    v_refs = refs[num_kv:2 * num_kv]
    o_ref = refs[2 * num_kv]
    tokens = q_ref.shape[0]
    scale = head_dim ** -0.5
    row_len = lens[0]
    last = num_kv - 1

    for head in range(num_q):
        cols = slice(head * head_dim, (head + 1) * head_dim)
        for qi in range(tokens // block):
            q = q_ref[qi * block:(qi + 1) * block, cols]
            scores = []
            for j in range(num_kv):
                width = tokens if j < last else (qi + 1) * block
                s = lax.dot_general(q, k_refs[j][:width, :], (((1,), (1,)), ((), ())), preferred_element_type=jnp.float32) * scale
                key_row = j * tokens + lax.broadcasted_iota(jnp.int32, (1, width), 1)
                if j < last:
                    visible = jnp.broadcast_to(key_row < row_len, s.shape)
                else:
                    key_pos = lax.broadcasted_iota(jnp.int32, s.shape, 1)
                    query_pos = qi * block + lax.broadcasted_iota(jnp.int32, s.shape, 0)
                    visible = (key_pos <= query_pos) & (key_row < row_len)
                scores.append(jnp.where(visible, s, -1e30))
            top = functools.reduce(jnp.maximum, [jnp.max(s, axis=-1, keepdims=True) for s in scores])
            weights = [jnp.exp(s - top) for s in scores]
            total = functools.reduce(jnp.add, [jnp.sum(w, axis=-1, keepdims=True) for w in weights])
            inverse = 1.0 / total
            out = None
            for j, w in enumerate(weights):
                part = jnp.dot((w * inverse).astype(jnp.bfloat16), v_refs[j][:w.shape[1], :], preferred_element_type=jnp.float32)
                out = part if out is None else out + part
            o_ref[qi * block:(qi + 1) * block, cols] = out.astype(jnp.bfloat16)


def attn_call(row_len, queries, keys, values, head_dim, num_q):
    tokens = queries.shape[0]
    num_kv = len(keys)
    full = lambda shape: pl.BlockSpec(shape, lambda i, s: (0,) * len(shape))
    return pl.pallas_call(
        functools.partial(attn_body, head_dim=head_dim, num_q=num_q, block=min(256, tokens)),
        grid_spec=pltpu.PrefetchScalarGridSpec(
            num_scalar_prefetch=1,
            grid=(1,),
            in_specs=[full(queries.shape)] + [full(keys[0].shape)] * (2 * num_kv),
            out_specs=full(queries.shape),
        ),
        out_shape=jax.ShapeDtypeStruct(queries.shape, jnp.bfloat16),
        compiler_params=pltpu.CompilerParams(vmem_limit_bytes=VMEM_BYTES),
        cost_estimate=pl.CostEstimate(flops=8 * num_q * tokens * tokens * num_kv * head_dim, bytes_accessed=4 * tokens * num_q * head_dim, transcendentals=num_q * tokens * tokens * num_kv),
        name="attn",
    )(row_len, queries, *keys, *values)


def ffn_body(place, h_ref, base_ref, *refs, tile, first, split_out):
    gate_p, up_p, down_p = refs[:6], refs[6:12], refs[12:18]
    refs = refs[18:]
    out_p = ()
    if first:
        out_p, refs = refs[:6], refs[6:]
    y_ref, gate_w, up_w, down_w, acc, sems = refs[:6]
    me = place[0]
    group = place[1]
    block = down_p[0].shape[1]
    ffn = down_p[0].shape[0]
    steps = ffn // tile
    half_steps = steps // 2
    offsets = row_offsets(me, group, gate_p[0].shape[0])
    blocks = [pl.ds(pl.multiple_of((me ^ i) * block, block), block) for i in range(4)]
    start = lambda copy: copy.start()
    wait = lambda copy: copy.wait()

    def fetch(f, slot, go):
        sem = sems.at[slot]
        cols = pl.ds(pl.multiple_of(f * tile, tile), tile)
        copies = piece_copies(gate_p, gate_w.at[slot], offsets, cols, sem)
        copies += piece_copies(up_p, up_w.at[slot], offsets, cols, sem)
        copies.append(pltpu.make_async_copy(down_p[0].at[cols], down_w.at[slot, :, blocks[0]], sem))
        copies.append(pltpu.make_async_copy(down_p[1].at[cols], down_w.at[slot, :, blocks[1]], sem))
        for copy in copies:
            go(copy)
        part = f // half_steps
        rows = pl.ds(pl.multiple_of((f - part * half_steps) * tile, tile), tile)
        for which in range(2):
            want = group if which == 0 else 1 - group

            @pl.when(part == want)
            def _():
                go(pltpu.make_async_copy(down_p[2 + which].at[rows], down_w.at[slot, :, blocks[2]], sem))
                go(pltpu.make_async_copy(down_p[4 + which].at[rows], down_w.at[slot, :, blocks[3]], sem))

    if first:
        out_w, out_sem = refs[6:]
        half = out_p[2].shape[0]
        near = pl.ds(pl.multiple_of(group * half, half), half)
        away = pl.ds(pl.multiple_of((1 - group) * half, half), half)
        out_copies = [
            pltpu.make_async_copy(out_p[0], out_w.at[:, blocks[0]], out_sem),
            pltpu.make_async_copy(out_p[1], out_w.at[:, blocks[1]], out_sem),
            pltpu.make_async_copy(out_p[2], out_w.at[near, blocks[2]], out_sem),
            pltpu.make_async_copy(out_p[3], out_w.at[away, blocks[2]], out_sem),
            pltpu.make_async_copy(out_p[4], out_w.at[near, blocks[3]], out_sem),
            pltpu.make_async_copy(out_p[5], out_w.at[away, blocks[3]], out_sem),
        ]
        for copy in out_copies:
            copy.start()
        fetch(0, 0, start)
        for copy in out_copies:
            copy.wait()
        acc[...] = jnp.dot(base_ref[...], out_w[...], preferred_element_type=jnp.float32)
    else:
        fetch(0, 0, start)
        acc[...] = base_ref[...]

    def step(f, carry):
        slot = lax.rem(f, 2)
        fetch(f, slot, wait)

        @pl.when(f + 1 < steps)
        def _():
            fetch(f + 1, 1 - slot, start)

        h = h_ref[...]
        gate = jnp.dot(h, gate_w[slot], preferred_element_type=jnp.float32)
        up = jnp.dot(h, up_w[slot], preferred_element_type=jnp.float32)
        act = (gate * jax.nn.sigmoid(gate) * up).astype(jnp.bfloat16)
        acc[...] += jnp.dot(act, down_w[slot], preferred_element_type=jnp.float32)
        return carry

    lax.fori_loop(0, steps, step, 0)
    if split_out:
        part = y_ref.shape[2]
        for j in range(y_ref.shape[0]):
            y_ref[j] = acc[:, j * part:(j + 1) * part].astype(y_ref.dtype)
    else:
        y_ref[...] = acc[...].astype(y_ref.dtype)


def ffn_call(place, normed, base, gate_p, up_p, down_p, out_p, split):
    first = out_p is not None
    tokens, embed = normed.shape
    ffn = down_p[0].shape[0]
    tile = min(FFN_TILE, ffn // 2)
    full = lambda shape: pl.BlockSpec(shape, lambda i, s: (0,) * len(shape))
    anyspec = pl.BlockSpec(memory_space=pl.ANY)
    bf16 = jnp.bfloat16
    out_dims = (split, tokens, embed // split) if split else (tokens, embed)
    scratch = [
        pltpu.VMEM((2, embed, tile), bf16),
        pltpu.VMEM((2, embed, tile), bf16),
        pltpu.VMEM((2, tile, embed), bf16),
        pltpu.VMEM((tokens, embed), jnp.float32),
        pltpu.SemaphoreType.DMA((2,)),
    ]
    if first:
        scratch += [pltpu.VMEM((base.shape[1], embed), bf16), pltpu.SemaphoreType.DMA]
    pieces = [*gate_p, *up_p, *down_p] + (list(out_p) if first else [])
    return pl.pallas_call(
        functools.partial(ffn_body, tile=tile, first=first, split_out=bool(split)),
        grid_spec=pltpu.PrefetchScalarGridSpec(
            num_scalar_prefetch=1,
            grid=(1,),
            in_specs=[full(normed.shape), full(base.shape)] + [anyspec] * len(pieces),
            out_specs=full(out_dims),
            scratch_shapes=scratch,
        ),
        out_shape=jax.ShapeDtypeStruct(out_dims, jnp.float32 if first else bf16),
        compiler_params=pltpu.CompilerParams(vmem_limit_bytes=VMEM_BYTES),
        cost_estimate=pl.CostEstimate(flops=2 * tokens * embed * 3 * ffn, bytes_accessed=2 * (2 * tokens * embed + 3 * ffn * embed), transcendentals=tokens * ffn),
    )(place, normed, base, *pieces)


def solution(mesh):
    m_size = mesh.shape['m']
    batch_axes = ('dp', 'bx')
    row_spec = P(batch_axes, None, 'm')
    cache_spec = P(None, batch_axes, None, None)
    in_specs = (row_spec, P(batch_axes), P(None, 'm'), P(None, 'bx', 'm'), P(None, 'bx', 'm'), P(None, 'bx', 'm', None), P(None, 'bx', None), P(None, 'bx', None), P(None, 'm', 'bx'), P(None, 'm', None, 'bx'))
    far_perm = [(b, b ^ 2) for b in range(4)]
    near_perm = [(b, b ^ 1) for b in range(4)]
    swap_perm = [(0, 1), (1, 0)]

    def spread(own, group):
        half = own.shape[0] // 2
        part = lax.dynamic_slice_in_dim(own, group * half, half, axis=0)
        far_a = lax.ppermute(part, 'bx', far_perm)
        far_b = lax.ppermute(far_a, 'dp', swap_perm)
        near = lax.ppermute(own, 'bx', near_perm)
        far_near_a = lax.ppermute(far_a, 'bx', near_perm)
        far_near_b = lax.ppermute(far_b, 'bx', near_perm)
        return own, near, far_a, far_b, far_near_a, far_near_b

    def gather_rows(own, col):
        pair = [(0, 1), (1, 0), (2, 3), (3, 2)]
        middle = [(1, 2), (2, 1)]
        outward = [(1, 0), (2, 3)]
        mate = lax.ppermute(own, 'm', pair)
        mid_own = lax.ppermute(own, 'm', middle)
        mid_mate = lax.ppermute(mate, 'm', middle)
        end_own = lax.ppermute(mid_own, 'm', outward)
        end_mate = lax.ppermute(mid_mate, 'm', outward)
        inner = (col == 1) | (col == 2)
        far_own = jnp.where(inner, mid_own, end_own)
        far_mate = jnp.where(inner, mid_mate, end_mate)
        pick = lambda a, b, c, d: jnp.where(col == 0, a, jnp.where(col == 1, b, jnp.where(col == 2, c, d)))
        return jnp.concatenate([
            pick(own, mate, far_mate, far_mate),
            pick(mate, own, far_own, far_own),
            pick(far_own, far_own, own, mate),
            pick(far_mate, far_mate, mate, own),
        ], axis=0)

    def layers(x_in, prompt_len, ln_scale, w_gate, w_up, w_q, w_k, w_v, w_down, w_o):
        x_own = x_in[0]
        seq, part_dim = x_own.shape
        embed = part_dim * m_size
        head_dim = w_k.shape[-1]
        num_q = w_q.shape[2]
        num_layers = w_gate.shape[0]
        tokens = seq // NUM_CHUNKS
        share = tokens // m_size
        half_ffn = w_gate.shape[2] // 2
        me = lax.axis_index('bx')
        group = lax.axis_index('dp')
        col = lax.axis_index('m')
        place = jnp.stack([me, group]).astype(jnp.int32)

        cos_tab, sin_tab = rotary_tables(jnp.arange(seq), head_dim)
        ln_full = lax.all_gather(ln_scale, 'm', axis=1, tiled=True)
        chunks = [lax.all_gather(x_own[c * tokens:(c + 1) * tokens], 'm', axis=0) for c in range(NUM_CHUNKS)]

        pieces = []
        for l in range(num_layers):
            own = {
                'qkv': jnp.concatenate([w_q[l].reshape(w_q.shape[1], -1), w_k[l], w_v[l]], axis=1),
                'out': w_o[l].reshape(-1, w_o.shape[-1]),
                'ga': w_gate[l, :, :half_ffn],
                'ua': w_up[l, :, :half_ffn],
                'da': w_down[l, :half_ffn],
                'gb': w_gate[l, :, half_ffn:],
                'ub': w_up[l, :, half_ffn:],
                'db': w_down[l, half_ffn:],
            }
            pieces.append({k: spread(v, group) for k, v in own.items()})

        def head(l, c, keys, values):
            rows = slice(c * tokens, (c + 1) * tokens)
            normed, q, k, v = qkv_call(place, chunks[c], ln_full[l:l + 1], cos_tab[rows], sin_tab[rows], pieces[l]['qkv'], head_dim, num_q)
            keys.append(k)
            values.append(v)
            return normed, attn_call(prompt_len, q, keys, values, head_dim, num_q)

        def ffn(l, normed, attn_out):
            w = pieces[l]
            half_sum = ffn_call(place, normed, attn_out, w['ga'], w['ua'], w['da'], w['out'], 0)
            return ffn_call(place, normed, half_sum, w['gb'], w['ub'], w['db'], None, m_size if l == 1 else 0)

        keys0, values0, keys1, values1 = [], [], [], []
        rows1 = []
        for c in range(NUM_CHUNKS):
            normed, attn_out = head(0, c, keys0, values0)
            partial = ffn(0, normed, attn_out)
            reduced = lax.psum_scatter(partial, 'm', scatter_dimension=0, tiled=True)
            before = lax.dynamic_slice_in_dim(chunks[c], col * share, share, axis=1)
            before = before.transpose(1, 0, 2).reshape(share, embed)
            y_rows = (before.astype(jnp.float32) + reduced.astype(jnp.float32)).astype(jnp.bfloat16)
            rows1.append(gather_rows(y_rows, col))
        chunks = rows1
        outs = []
        for c in range(NUM_CHUNKS):
            normed, attn_out = head(1, c, keys1, values1)
            partial = ffn(1, normed, attn_out)
            reduced = lax.psum_scatter(partial, 'm', scatter_dimension=0, tiled=True)
            before = lax.dynamic_slice_in_dim(chunks[c], col * part_dim, part_dim, axis=1)
            outs.append((before.astype(jnp.float32) + reduced[0].astype(jnp.float32)).astype(jnp.bfloat16))
        hidden = jnp.concatenate(outs, axis=0)[None]
        k_cache = jnp.stack([jnp.concatenate(keys0, axis=0), jnp.concatenate(keys1, axis=0)])[:, None]
        v_cache = jnp.stack([jnp.concatenate(values0, axis=0), jnp.concatenate(values1, axis=0)])[:, None]
        return hidden, k_cache, v_cache

    return jax.shard_map(layers, mesh=mesh, in_specs=in_specs, out_specs=(row_spec, cache_spec, cache_spec), check_vma=False)
```
